32 devices in a mesh: dp: 4 (over x, core), context: 2 (over y), tensor: 4 (over z).
Axes of the slice: x: 2, y: 2, z: 4, core: 2. Of those that a mesh axis runs over, the one named last changes fastest.
Arguments:
- tokens: bfloat16 [12, 512, 1536], P('dp', 'context')
- cotangent: bfloat16 [12, 512, 1536], P('dp', 'context'), may hold values from -6 to 6
- segments: int32 [12, 512], P('dp'), may hold values from 0 to 3, as said below
- positions: int32 [12, 512], P('dp', 'context'), may hold values from 0 to 255, as said below
- norm_attn: bfloat16 [1536], replicated, may hold values from 0.099609375 to 1.8984375
- w_query: bfloat16 [1536, 1536], P(None, 'tensor')
- key_weight: bfloat16 [1536, 768], P(None, 'tensor')
- value_weight: bfloat16 [1536, 768], P(None, 'tensor'), may hold values from -0.15625 to 0.15625
- w_out: bfloat16 [1536, 1536], P('tensor'), may hold values from -0.875 to 0.875
- norm_ffn: bfloat16 [1536], replicated, may hold values from 0.099609375 to 1.8984375
- w_gate: bfloat16 [1536, 4096], P(None, 'tensor'), may hold values from -0.15625 to 0.15625
- w_up: bfloat16 [1536, 4096], P(None, 'tensor'), may hold values from -0.15625 to 0.15625
- w_down: bfloat16 [4096, 1536], P('tensor'), may hold values from -0.09375 to 0.09375
Outputs:
- block_out: bfloat16 [12, 512, 1536], P('dp', 'context')
- input_grad: bfloat16 [12, 512, 1536], P('dp', 'context')
- attn_gain_grad: float32 [1536], replicated
- query_grad: float32 [1536, 1536], P(None, 'tensor')
- key_grad: float32 [1536, 768], P(None, 'tensor')
- value_grad: float32 [1536, 768], P(None, 'tensor')
- out_grad: float32 [1536, 1536], P('tensor')
- ffn_gain_grad: float32 [1536], replicated
- gate_grad: float32 [1536, 4096], P(None, 'tensor')
- up_grad: float32 [1536, 4096], P(None, 'tensor')
- down_grad: float32 [4096, 1536], P('tensor')
The draws below stay inside these ranges and needn't reach their ends.
Inputs may be any that keep to these rules, and one draw needn't show every extreme that they name: `segments`: each sequence holds exactly four documents, numbered from 0 on its first token, never falling and rising by one at the first token of each further document; one of the four is 256 tokens long and the others are shorter. `positions`: each token's position is its offset from the first token of its document in its sequence.
All inputs are finite; a program needn't handle non-finite values.
Results may differ from the reference program's by a relative error of at most 0.019.
Values may be sent and summed in bfloat16 or wider, within the bound.
A program may use at most 192 MiB of HBM per device.

```python
import math
from functools import partial
import jax
import jax.numpy as jnp
from jax import lax

MODEL_DIMENSION = 1536
QUERY_HEADS = 16
KEY_VALUE_HEADS = 8
HEAD_SIZE = 96
FEEDFORWARD_SIZE = 4096
PACKED_LENGTH = 512
SEQS = 12
N_TENSOR = 4


def layout_one(key):
    half_len = PACKED_LENGTH // 2
    cut_pair = jax.random.permutation(jax.random.fold_in(key, 1), half_len - 1)[:2].astype(jnp.int32) + 1
    first_cut = jnp.minimum(cut_pair[0], cut_pair[1])
    second_cut = jnp.maximum(cut_pair[0], cut_pair[1])
    short_lens = jnp.stack([first_cut, second_cut - first_cut, half_len - second_cut]).astype(jnp.int32)
    long_slot = jax.random.randint(jax.random.fold_in(key, 2), (), 0, 4).astype(jnp.int32)
    slot_index = jnp.arange(4, dtype=jnp.int32)
    before = short_lens[jnp.minimum(slot_index, 2)]
    after = short_lens[jnp.maximum(slot_index - 1, 0)]
    doc_lens = jnp.where(slot_index < long_slot, before, jnp.where(slot_index == long_slot, half_len, after)).astype(jnp.int32)
    doc_ends = jnp.cumsum(doc_lens).astype(jnp.int32)
    doc_starts = (doc_ends - doc_lens).astype(jnp.int32)
    index_row = jnp.arange(PACKED_LENGTH, dtype=jnp.int32)
    segment_ids = jnp.sum((index_row[:, None] >= doc_ends[None, :3]).astype(jnp.int32), axis=1).astype(jnp.int32)
    start_of = jnp.sum(jnp.where(segment_ids[:, None] == slot_index[None, :], doc_starts[None, :], 0), axis=1).astype(jnp.int32)
    return (segment_ids, (index_row - start_of).astype(jnp.int32))


def doc_layout(key):
    inner = jax.random.fold_in(key, 11)
    seq_keys = jax.random.split(inner, SEQS)
    return jax.vmap(layout_one)(seq_keys)


def draw_segments(key, part):
    return doc_layout(key)[0]


def draw_positions(key, part):
    return doc_layout(key)[1]


def draw_tokens(key, part):
    shape_full = (SEQS, PACKED_LENGTH, MODEL_DIMENSION)
    noise = jax.random.normal(jax.random.fold_in(key, 1), shape_full, jnp.float32)
    row_scale = jnp.exp(jax.random.uniform(jax.random.fold_in(key, 2), (SEQS, PACKED_LENGTH, 1), jnp.float32, math.log(0.5), math.log(5.0)))
    column_scale = jnp.exp(jax.random.uniform(jax.random.fold_in(key, 3), (MODEL_DIMENSION,), jnp.float32, math.log(0.4), math.log(4.0)))
    return (noise * row_scale * column_scale).astype(jnp.bfloat16)


def projection_draw(key, shape_full):
    sampled_values = jax.random.normal(key, shape_full, jnp.float32)
    return (sampled_values * (1.0 / math.sqrt(MODEL_DIMENSION))).astype(jnp.bfloat16)


def draw_w_query(key, part):
    return projection_draw(key, (MODEL_DIMENSION, QUERY_HEADS * HEAD_SIZE))


def draw_key_weight(key, part):
    return projection_draw(key, (MODEL_DIMENSION, KEY_VALUE_HEADS * HEAD_SIZE))


def levels(own_key, extent, cuts, smallest, high):
    loudness, own = 1.0, jax.random.fold_in(own_key, 6)
    for dim, parts in cuts:
        steps = jnp.exp(jax.random.uniform(jax.random.fold_in(own, dim), (parts,), jnp.float32, smallest / len(cuts), high / len(cuts)))
        loudness = loudness * jnp.repeat(steps, extent[dim] // parts).reshape([-1 if axis == dim else 1 for axis in range(len(extent))])
    return loudness


def gaussian(key, dims, deviation, limit, pieces=(), kind=jnp.bfloat16):
    drawn = deviation * jax.random.normal(key, dims, jnp.float32)
    if pieces:
        drawn = drawn * levels(key, dims, pieces, -0.22, 0.18)
    return jnp.clip(drawn, -limit, limit).astype(kind)


def setup_inputs(seed: int = 0) -> dict:
    splits = jax.random.split(jax.random.key(seed), 14)
    return {
        "tokens": draw_tokens(jax.random.fold_in(splits[13], 71), 0),
        "cotangent": gaussian(splits[1], (SEQS, PACKED_LENGTH, MODEL_DIMENSION), 1.0, 6.0, ((0, 4), (1, 2))),
        "segments": draw_segments(jax.random.fold_in(splits[13], 71), 0),
        "positions": draw_positions(jax.random.fold_in(splits[13], 71), 0),
        "norm_attn": jnp.clip(1.0 + 0.18 * jax.random.normal(splits[4], (MODEL_DIMENSION,), jnp.float32), 0.099609375, 1.8984375).astype(jnp.bfloat16),
        "w_query": draw_w_query(jax.random.fold_in(splits[13], 71), 0),
        "key_weight": draw_key_weight(jax.random.fold_in(splits[13], 71), 0),
        "value_weight": gaussian(splits[7], (MODEL_DIMENSION, KEY_VALUE_HEADS * HEAD_SIZE), MODEL_DIMENSION ** -0.5, 0.15625, ((1, 4),)),
        "w_out": gaussian(splits[8], (QUERY_HEADS * HEAD_SIZE, MODEL_DIMENSION), (QUERY_HEADS * HEAD_SIZE // 32) ** -0.5, 0.875, ((0, 4),)),
        "norm_ffn": jnp.clip(1.0 + 0.18 * jax.random.normal(splits[9], (MODEL_DIMENSION,), jnp.float32), 0.099609375, 1.8984375).astype(jnp.bfloat16),
        "w_gate": gaussian(splits[10], (MODEL_DIMENSION, FEEDFORWARD_SIZE), MODEL_DIMENSION ** -0.5, 0.15625, ((1, 4),)),
        "w_up": gaussian(splits[11], (MODEL_DIMENSION, FEEDFORWARD_SIZE), MODEL_DIMENSION ** -0.5, 0.15625, ((1, 4),)),
        "w_down": gaussian(splits[12], (FEEDFORWARD_SIZE, MODEL_DIMENSION), FEEDFORWARD_SIZE ** -0.5, 0.09375, ((0, 4),)),
    }


EPS = 1e-05
THETA = 100000.0

def rope_tables(position_row):
    steps_half = jnp.arange(HEAD_SIZE // 2).astype(jnp.float32)
    inverse = THETA ** (-2.0 * steps_half / HEAD_SIZE)
    angles = position_row.astype(jnp.float32)[:, None] * inverse[None, :]
    return (jnp.cos(angles), jnp.sin(angles))

def apply_rotary(operand, cosine, sine_part):
    half_width = operand.shape[-1] // 2
    lead_half = operand[..., :half_width]
    tail_half = operand[..., half_width:]
    return jnp.concatenate([lead_half * cosine - tail_half * sine_part, tail_half * cosine + lead_half * sine_part], axis=-1)

def inverse_rotary(operand, cosine, sine_part):
    half_width = operand.shape[-1] // 2
    lead_half = operand[..., :half_width]
    tail_half = operand[..., half_width:]
    return jnp.concatenate([lead_half * cosine + tail_half * sine_part, tail_half * cosine - lead_half * sine_part], axis=-1)

def round_trip(operand):
    return lax.optimization_barrier(operand.astype(jnp.bfloat16)).astype(jnp.float32)

def group_sum(pairs, pattern):
    partials = jnp.einsum(pattern, pairs[0][0], pairs[0][1])
    for left_side, right_side in pairs[1:]:
        partials = partials + jnp.einsum(pattern, left_side, right_side)
    return lax.optimization_barrier(jnp.sum(round_trip(partials), axis=0))

def head_scores(query_head, key_head, allowed):
    scores = jnp.einsum('igd,jd->gij', query_head.astype(jnp.float32), key_head.astype(jnp.float32)) * (1.0 / math.sqrt(HEAD_SIZE))
    return scores

def head_forward(operands, allowed):
    query_head, key_head, value_head = operands
    scores = head_scores(query_head, key_head, allowed)
    masked = jnp.where(allowed[None], scores, -jnp.inf)
    top_value = lax.optimization_barrier(jnp.max(masked, axis=-1, keepdims=True))
    total = lax.optimization_barrier(jnp.sum(jnp.where(allowed[None], jnp.exp(masked - top_value), 0.0), axis=-1, keepdims=True))
    log_total = top_value + jnp.log(total)
    weights = jnp.where(allowed[None], jnp.exp(scores - log_total), 0.0)
    attended = jnp.einsum('gij,jd->igd', round_trip(weights), value_head.astype(jnp.float32))
    return (attended.astype(jnp.bfloat16), log_total)

def head_backward(operands, allowed):
    query_head, key_head, value_head, head_gradient, head_dot_grad, log_total = operands
    scores = head_scores(query_head, key_head, allowed)
    weights = jnp.where(allowed[None], jnp.exp(scores - log_total), 0.0)
    prob_grad = jnp.einsum('igd,jd->gij', head_gradient.astype(jnp.float32), value_head.astype(jnp.float32))
    score_grad = round_trip(weights * (prob_grad - head_dot_grad[..., None]) * (1.0 / math.sqrt(HEAD_SIZE)))
    query_rot = jnp.einsum('gij,jd->igd', score_grad, key_head.astype(jnp.float32))
    key_rotated = jnp.einsum('gij,igd->jd', score_grad, query_head.astype(jnp.float32))
    value_unscaled = jnp.einsum('gij,igd->jd', round_trip(weights), head_gradient.astype(jnp.float32))
    return (query_rot, key_rotated, value_unscaled)

def reference(tokens, cotangent, segments, positions, norm_attn, w_query, key_weight, value_weight, w_out, norm_ffn, w_gate, w_up, w_down):
    single_float = jnp.float32
    brain_float_half = jnp.bfloat16
    group_of_head = QUERY_HEADS // KEY_VALUE_HEADS

    def dot_single_precision(left_side, right_side):
        return jnp.dot(left_side, right_side, preferred_element_type=jnp.float32)

    def one_sequence(carry, inputs):
        tok_row, cot_row, segment_row, position_row = inputs
        tok_f = tok_row.astype(single_float)
        inv_attn = lax.rsqrt(lax.optimization_barrier(jnp.mean(tok_f * tok_f, axis=-1, keepdims=True)) + EPS)
        normalized_attention_input = (tok_f * inv_attn * norm_attn.astype(single_float)).astype(brain_float_half)
        cosine, sine_part = rope_tables(position_row)
        cosine_per_head = cosine[:, None, :]
        sine_per_head = sine_part[:, None, :]
        query_rows = apply_rotary(dot_single_precision(normalized_attention_input, w_query).reshape(PACKED_LENGTH, QUERY_HEADS, HEAD_SIZE), cosine_per_head, sine_per_head).astype(brain_float_half)
        key_rows = apply_rotary(dot_single_precision(normalized_attention_input, key_weight).reshape(PACKED_LENGTH, KEY_VALUE_HEADS, HEAD_SIZE), cosine_per_head, sine_per_head).astype(brain_float_half)
        value_rows = dot_single_precision(normalized_attention_input, value_weight).astype(brain_float_half).reshape(PACKED_LENGTH, KEY_VALUE_HEADS, HEAD_SIZE)
        index_row = jnp.arange(PACKED_LENGTH, dtype=jnp.int32)
        allowed = (segment_row[None, :] == segment_row[:, None]) & (index_row[None, :] <= index_row[:, None])
        grouped_rows = query_rows.reshape(PACKED_LENGTH, KEY_VALUE_HEADS, group_of_head, HEAD_SIZE).transpose(1, 0, 2, 3)
        keys_head = key_rows.transpose(1, 0, 2)
        values_head = value_rows.transpose(1, 0, 2)
        attended_head, log_total = lax.map(partial(head_forward, allowed=allowed), (grouped_rows, keys_head, values_head))
        attended = attended_head.transpose(1, 0, 2, 3).reshape(PACKED_LENGTH, QUERY_HEADS * HEAD_SIZE)
        attn_total = group_sum([(attended.astype(single_float).reshape(PACKED_LENGTH, N_TENSOR, -1), w_out.astype(single_float).reshape(N_TENSOR, -1, MODEL_DIMENSION))], 'ltc,tcd->tld')
        hidden_res = tok_f + attn_total
        inv_ffn = lax.rsqrt(lax.optimization_barrier(jnp.mean(hidden_res * hidden_res, axis=-1, keepdims=True)) + EPS)
        normed_ffn = (hidden_res * inv_ffn * norm_ffn.astype(single_float)).astype(brain_float_half)
        gate_proj = dot_single_precision(normed_ffn, w_gate)
        up_proj = dot_single_precision(normed_ffn, w_up)
        sigmoid_gate = jax.nn.sigmoid(gate_proj)
        silu_gate = gate_proj * sigmoid_gate
        activated = (silu_gate * up_proj).astype(brain_float_half)
        ffn_total = group_sum([(activated.astype(single_float).reshape(PACKED_LENGTH, N_TENSOR, -1), w_down.astype(single_float).reshape(N_TENSOR, -1, MODEL_DIMENSION))], 'ltc,tcd->tld')
        block_out = (hidden_res + ffn_total).astype(brain_float_half)
        cot_f = cot_row.astype(single_float)
        down_grad = dot_single_precision(activated.T, cot_row)
        grad_act = dot_single_precision(cot_row, w_down.T)
        grad_gate = (grad_act * up_proj * sigmoid_gate * (1.0 + gate_proj * (1.0 - sigmoid_gate))).astype(brain_float_half)
        grad_up = (grad_act * silu_gate).astype(brain_float_half)
        gate_grad = dot_single_precision(normed_ffn.T, grad_gate)
        up_grad = dot_single_precision(normed_ffn.T, grad_up)
        grad_normed_ffn = group_sum([(grad_gate.astype(single_float).reshape(PACKED_LENGTH, N_TENSOR, -1), w_gate.astype(single_float).reshape(MODEL_DIMENSION, N_TENSOR, -1)), (grad_up.astype(single_float).reshape(PACKED_LENGTH, N_TENSOR, -1), w_up.astype(single_float).reshape(MODEL_DIMENSION, N_TENSOR, -1))], 'ltc,dtc->tld')
        ffn_gain_grad = lax.optimization_barrier(jnp.sum(grad_normed_ffn * hidden_res * inv_ffn, axis=0))
        scaled_ffn = grad_normed_ffn * norm_ffn.astype(single_float)
        grad_hidden = cot_f + inv_ffn * scaled_ffn - hidden_res * inv_ffn ** 3 * lax.optimization_barrier(jnp.mean(scaled_ffn * hidden_res, axis=-1, keepdims=True))
        grad_hidden_b = grad_hidden.astype(brain_float_half)
        out_grad = dot_single_precision(attended.T, grad_hidden_b)
        attended_gradient = dot_single_precision(grad_hidden_b, w_out.T).astype(brain_float_half)
        output_dot_grad = lax.optimization_barrier(jnp.sum(attended_gradient.astype(single_float).reshape(PACKED_LENGTH, QUERY_HEADS, HEAD_SIZE) * attended.astype(single_float).reshape(PACKED_LENGTH, QUERY_HEADS, HEAD_SIZE), axis=-1))
        head_dot_grad = output_dot_grad.reshape(PACKED_LENGTH, KEY_VALUE_HEADS, group_of_head).transpose(1, 2, 0)
        head_gradient = attended_gradient.reshape(PACKED_LENGTH, KEY_VALUE_HEADS, group_of_head, HEAD_SIZE).transpose(1, 0, 2, 3)
        query_rot, key_rotated, value_unscaled = lax.map(partial(head_backward, allowed=allowed), (grouped_rows, keys_head, values_head, head_gradient, head_dot_grad, log_total))
        query_rot = query_rot.transpose(1, 0, 2, 3).reshape(PACKED_LENGTH, QUERY_HEADS, HEAD_SIZE)
        query_lin = inverse_rotary(query_rot, cosine_per_head, sine_per_head).astype(brain_float_half).reshape(PACKED_LENGTH, QUERY_HEADS * HEAD_SIZE)
        key_linear = inverse_rotary(key_rotated.transpose(1, 0, 2), cosine_per_head, sine_per_head).astype(brain_float_half).reshape(PACKED_LENGTH, KEY_VALUE_HEADS * HEAD_SIZE)
        value_linear = value_unscaled.transpose(1, 0, 2).astype(brain_float_half).reshape(PACKED_LENGTH, KEY_VALUE_HEADS * HEAD_SIZE)
        query_grad = dot_single_precision(normalized_attention_input.T, query_lin)
        key_grad = dot_single_precision(normalized_attention_input.T, key_linear)
        value_grad = dot_single_precision(normalized_attention_input.T, value_linear)
        grad_normed_attn = group_sum([(query_lin.astype(single_float).reshape(PACKED_LENGTH, N_TENSOR, -1), w_query.astype(single_float).reshape(MODEL_DIMENSION, N_TENSOR, -1)), (key_linear.astype(single_float).reshape(PACKED_LENGTH, N_TENSOR, -1), key_weight.astype(single_float).reshape(MODEL_DIMENSION, N_TENSOR, -1)), (value_linear.astype(single_float).reshape(PACKED_LENGTH, N_TENSOR, -1), value_weight.astype(single_float).reshape(MODEL_DIMENSION, N_TENSOR, -1))], 'ltc,dtc->tld')
        attn_gain_grad = lax.optimization_barrier(jnp.sum(grad_normed_attn * tok_f * inv_attn, axis=0))
        scaled_attn = grad_normed_attn * norm_attn.astype(single_float)
        input_grad = grad_hidden + inv_attn * scaled_attn - tok_f * inv_attn ** 3 * lax.optimization_barrier(jnp.mean(scaled_attn * tok_f, axis=-1, keepdims=True))
        updates = (attn_gain_grad, query_grad, key_grad, value_grad, out_grad, ffn_gain_grad, gate_grad, up_grad, down_grad)
        carry = tuple((old + new for old, new in zip(carry, updates)))
        return (carry, (block_out, input_grad.astype(brain_float_half)))
    start_position = (jnp.zeros((MODEL_DIMENSION,), single_float), jnp.zeros((MODEL_DIMENSION, QUERY_HEADS * HEAD_SIZE), single_float), jnp.zeros((MODEL_DIMENSION, KEY_VALUE_HEADS * HEAD_SIZE), single_float), jnp.zeros((MODEL_DIMENSION, KEY_VALUE_HEADS * HEAD_SIZE), single_float), jnp.zeros((QUERY_HEADS * HEAD_SIZE, MODEL_DIMENSION), single_float), jnp.zeros((MODEL_DIMENSION,), single_float), jnp.zeros((MODEL_DIMENSION, FEEDFORWARD_SIZE), single_float), jnp.zeros((MODEL_DIMENSION, FEEDFORWARD_SIZE), single_float), jnp.zeros((FEEDFORWARD_SIZE, MODEL_DIMENSION), single_float))
    sums, outputs = lax.scan(one_sequence, start_position, (tokens, cotangent, segments, positions))
    block_out, input_grad = outputs
    return (block_out, input_grad, sums[0], sums[1], sums[2], sums[3], sums[4], sums[5], sums[6], sums[7], sums[8])
```

```python
import functools
import math

import jax
import jax.numpy as jnp
from jax import lax
from jax.experimental import pallas as pl
from jax.experimental.pallas import tpu as pltpu
from jax.sharding import PartitionSpec as P

HEAD = 96
PAD = 128
EPS = 1e-05
THETA = 100000.0
NEG = -1e30
F32 = jnp.float32
BF16 = jnp.bfloat16
MESH = pl.DeviceIdType.MESH
VMEM = pltpu.MemorySpace.VMEM
HALVES = 2


def mm(a, b):
    return jnp.dot(a, b, preferred_element_type=F32)


def mm_nt(a, b):
    return lax.dot_general(a, b, (((1,), (1,)), ((), ())), preferred_element_type=F32)


def mm_tn(a, b):
    return lax.dot_general(a, b, (((0,), (0,)), ((), ())), preferred_element_type=F32)


class Line:
    def __init__(self, axis, part, rbuf, full, rs_send, rs_recv, ag_send, ag_recv):
        self.axis = axis
        self.n = lax.axis_size(axis)
        self.me = lax.axis_index(axis)
        self.part, self.rbuf, self.full = part, rbuf, full
        self.rs_send, self.rs_recv = rs_send, rs_recv
        self.ag_send, self.ag_recv = ag_send, ag_recv

    def rs_copy(self, u, side, j):
        n = self.n
        slot = j - 1 if side == 0 else j
        return pltpu.make_async_remote_copy(
            src_ref=self.part.at[u, j],
            dst_ref=self.rbuf.at[u, side, slot],
            send_sem=self.rs_send.at[u, side, slot],
            recv_sem=self.rs_recv.at[u, side, slot],
            device_id={self.axis: self.me + (1 if side == 0 else -1)},
            device_id_type=MESH,
        )

    def rs_start(self, u):
        n, me = self.n, self.me

        @pl.when(me == 0)
        def _():
            for j in range(n - 1, 0, -1):
                self.rs_copy(u, 0, j).start()

        @pl.when(me == n - 1)
        def _():
            for j in range(n - 1):
                self.rs_copy(u, 1, j).start()

    def rs_step(self, u, t):
        n, me = self.n, self.me
        j = n - 1 - t

        @pl.when((me > 0) & (me <= j))
        def _():
            self.rs_copy(u, 0, j).wait_recv()

        @pl.when((me > 0) & (me < j))
        def _():
            self.part[u, j] = (
                self.part[u, j].astype(F32) + self.rbuf[u, 0, j - 1].astype(F32)
            ).astype(BF16)
            self.rs_copy(u, 0, j).start()

        k = t

        @pl.when((me < n - 1) & (me >= k))
        def _():
            self.rs_copy(u, 1, k).wait_recv()

        @pl.when((me < n - 1) & (me > k))
        def _():
            self.part[u, k] = (
                self.part[u, k].astype(F32) + self.rbuf[u, 1, k].astype(F32)
            ).astype(BF16)
            self.rs_copy(u, 1, k).start()

    def rs_own(self, u, out):
        n, me = self.n, self.me
        out[...] = self.part[u, me].astype(F32)

        @pl.when(me > 0)
        def _():
            out[...] += self.rbuf[u, 0, me - 1].astype(F32)

        @pl.when(me < n - 1)
        def _():
            out[...] += self.rbuf[u, 1, me].astype(F32)

    def rs_drain(self, u):
        n, me = self.n, self.me
        for j in range(1, n):

            @pl.when(me < j)
            def _():
                self.rs_copy(u, 0, j).wait_send()

        for j in range(n - 1):

            @pl.when(me > j)
            def _():
                self.rs_copy(u, 1, j).wait_send()

    def ag_copy(self, u, side, j):
        return pltpu.make_async_remote_copy(
            src_ref=self.full.at[u, j],
            dst_ref=self.full.at[u, j],
            send_sem=self.ag_send.at[u, side, j],
            recv_sem=self.ag_recv.at[u, side, j],
            device_id={self.axis: self.me + (1 if side == 0 else -1)},
            device_id_type=MESH,
        )

    def ag_start(self, u):
        n, me = self.n, self.me

        @pl.when(me < n - 1)
        def _():
            self.ag_copy(u, 0, me).start()

        @pl.when(me > 0)
        def _():
            self.ag_copy(u, 1, me).start()

    def ag_step(self, u, s):
        n, me = self.n, self.me

        @pl.when(me - s >= 0)
        def _():
            self.ag_copy(u, 0, me - s).wait_recv()

        @pl.when((me - s >= 0) & (me < n - 1))
        def _():
            self.ag_copy(u, 0, me - s).start()

        @pl.when(me + s <= n - 1)
        def _():
            self.ag_copy(u, 1, me + s).wait_recv()

        @pl.when((me + s <= n - 1) & (me > 0))
        def _():
            self.ag_copy(u, 1, me + s).start()

    def ag_drain(self, u):
        n, me = self.n, self.me
        for j in range(n):

            @pl.when((j <= me) & (me < n - 1))
            def _():
                self.ag_copy(u, 0, j).wait_send()

            @pl.when((j >= me) & (me > 0))
            def _():
                self.ag_copy(u, 1, j).wait_send()


def line_sems(units, n):
    return [
        pltpu.SemaphoreType.DMA((units, 2, n - 1)),
        pltpu.SemaphoreType.DMA((units, 2, n - 1)),
        pltpu.SemaphoreType.DMA((units, 2, n)),
        pltpu.SemaphoreType.DMA((units, 2, n)),
    ]


def enter(context_peers):
    n, me = lax.axis_size("tensor"), lax.axis_index("tensor")
    slices, mine = lax.axis_size("context"), lax.axis_index("context")
    barrier = pltpu.get_barrier_semaphore()

    @pl.when(me > 0)
    def _():
        pl.semaphore_signal(barrier, inc=1, device_id={"tensor": me - 1}, device_id_type=MESH)

    @pl.when(me < n - 1)
    def _():
        pl.semaphore_signal(barrier, inc=1, device_id={"tensor": me + 1}, device_id_type=MESH)

    for d in range(1, slices):

        @pl.when(mine + d < slices)
        def _():
            pl.semaphore_signal(
                barrier, inc=1, device_id={"context": mine + d}, device_id_type=MESH
            )

        @pl.when(mine - d >= 0)
        def _():
            pl.semaphore_signal(
                barrier, inc=1, device_id={"context": mine - d}, device_id_type=MESH
            )

    @pl.when((me > 0) & (me < n - 1))
    def _():
        pl.semaphore_wait(barrier, slices + 1)

    @pl.when((me == 0) | (me == n - 1))
    def _():
        pl.semaphore_wait(barrier, slices)


def lane_of(shape):
    return lax.broadcasted_iota(jnp.int32, shape, len(shape) - 1)


def swap_halves(x):
    width = x.shape[-1]
    half = HEAD // 2
    first = (lane_of(x.shape) % HEAD) < half
    return jnp.where(first, pltpu.roll(x, width - half, 1), pltpu.roll(x, half, 1))


def take_head(x, h):
    width = x.shape[-1]
    moved = x if h == 0 else pltpu.roll(x, width - h * HEAD, 1)
    moved = moved[:, :PAD]
    return jnp.where(lane_of(moved.shape) < HEAD, moved, 0.0)


def put_heads(pieces, width):
    rows = pieces[0].shape[0]
    total = None
    for h, piece in enumerate(pieces):
        wide = jnp.concatenate([piece, jnp.zeros((rows, width - PAD), F32)], axis=1)
        wide = wide if h == 0 else pltpu.roll(wide, h * HEAD, 1)
        total = wide if total is None else total + wide
    return total


def mask_of(qseg, kseg, diagonal):
    ok = qseg == kseg
    if diagonal:
        shape = ok.shape
        ok = ok & (
            lax.broadcasted_iota(jnp.int32, shape, 1) <= lax.broadcasted_iota(jnp.int32, shape, 0)
        )
    return ok


def twice(ok):
    bias = jnp.where(ok, 0.0, NEG)
    return jnp.concatenate([bias, bias], axis=0)


def forward_kernel(
    seqs,
    tokens,
    cot,
    qseg,
    kseg,
    na,
    nf,
    wqkv,
    w_out,
    w_gate,
    w_up,
    w_down,
    cos,
    sin,
    normed_attn,
    qpad,
    kv,
    lse,
    attended,
    attpad,
    hidden_own,
    normed_ffn,
    act,
    ggate,
    gup,
    ffn_part,
    gh_own,
    ghb,
    ffn_gain,
    part_a,
    rbuf_a,
    part_c,
    rbuf_c,
    gact,
    own,
    a_rs_s,
    a_rs_r,
    a_ag_s,
    a_ag_r,
    c_rs_s,
    c_rs_r,
    c_ag_s,
    c_ag_r,
    kv_s,
    kv_r,
):
    n = lax.axis_size("tensor")
    me = lax.axis_index("tensor")
    slices, mine = lax.axis_size("context"), lax.axis_index("context")
    rows = tokens.shape[0] // seqs
    width = tokens.shape[1]
    qw = w_out.shape[0]
    heads = qw // HEAD
    kvh = heads // 2
    pairw = wqkv.shape[1] - qw
    hidden = w_gate.shape[1]
    shard = rows // HALVES // n
    scale = 1.0 / math.sqrt(HEAD)
    line_a = Line("tensor", part_a, rbuf_a, normed_ffn, a_rs_s, a_rs_r, a_ag_s, a_ag_r)
    line_c = Line("tensor", part_c, rbuf_c, ghb, c_rs_s, c_rs_r, c_ag_s, c_ag_r)
    enter(True)

    def rows_of(c):
        return pl.ds(c * rows, rows)

    def kv_copy(c, d):
        return pltpu.make_async_remote_copy(
            src_ref=kv.at[c, mine],
            dst_ref=kv.at[c, mine],
            send_sem=kv_s.at[c, d - 1],
            recv_sem=kv_r.at[c, d - 1],
            device_id={"context": mine + d},
            device_id_type=MESH,
        )

    def project(c):
        x = tokens[rows_of(c), :].astype(F32)
        inv = lax.rsqrt(jnp.mean(x * x, axis=-1, keepdims=True) + EPS)
        normed = (x * inv * na[...]).astype(BF16)
        normed_attn[rows_of(c), :] = normed
        ct, st = cos[rows_of(c), :], sin[rows_of(c), :]
        q = mm(normed, wqkv[:, :qw])
        q = q * ct + swap_halves(q) * st
        for h in range(heads):
            qpad[c, h] = take_head(q, h).astype(BF16)
        p = mm(normed, wqkv[:, qw:])
        roped = p * ct[:, :pairw] + swap_halves(p) * st[:, :pairw]
        p = jnp.where(lane_of(p.shape) < kvh * HEAD, roped, p)
        for h in range(2 * kvh):
            kv[c, mine, h] = take_head(p, h).astype(BF16)
        for d in range(1, slices):

            @pl.when(mine + d < slices)
            def _():
                kv_copy(c, d).start()

    def attend(c):
        for d in range(1, slices):

            @pl.when(mine - d >= 0)
            def _():
                pltpu.make_async_remote_copy(
                    src_ref=kv.at[c, mine - d],
                    dst_ref=kv.at[c, mine - d],
                    send_sem=kv_s.at[c, d - 1],
                    recv_sem=kv_r.at[c, d - 1],
                    device_id={"context": mine - d},
                    device_id_type=MESH,
                ).wait_recv()

        qs = qseg[c]
        outs = []
        bias0 = twice(mask_of(qs, kseg[c, mine], True))
        for g in range(kvh):
            q2 = qpad[c, 2 * g : 2 * g + 2].reshape(2 * rows, PAD)
            s = mm_nt(q2, kv[c, mine, g]) * scale + bias0
            m = jnp.max(s, axis=-1, keepdims=True)
            p = jnp.exp(s - m)
            l = jnp.sum(p, axis=-1, keepdims=True)
            acc = mm(p.astype(BF16), kv[c, mine, kvh + g])

            def block(b, carry):
                m, l, acc = carry
                bias = twice(mask_of(qs, kseg[c, b], False))
                s = mm_nt(q2, kv[c, b, g]) * scale + bias
                m2 = jnp.maximum(m, jnp.max(s, axis=-1, keepdims=True))
                alpha = jnp.exp(m - m2)
                p = jnp.exp(s - m2)
                return (
                    m2,
                    l * alpha + jnp.sum(p, axis=-1, keepdims=True),
                    acc * alpha + mm(p.astype(BF16), kv[c, b, kvh + g]),
                )

            m, l, acc = lax.fori_loop(0, mine, block, (m, l, acc))
            lse[c, g] = m + jnp.log(l)
            out = acc / l
            outs += [out[:rows], out[rows:]]
        for h in range(heads):
            attpad[c, h] = outs[h].astype(BF16)
        attended[rows_of(c), :] = put_heads(outs, qw).astype(BF16)

    def units(c):
        return range(c * HALVES, (c + 1) * HALVES)

    def store_part(part, c, col, wide, value):
        part[pl.ds(c * HALVES, HALVES), :, :, pl.ds(col, wide)] = value.astype(BF16).reshape(
            HALVES, n, shard, wide
        )

    step = 512

    def out_project(c):
        a = attended[rows_of(c), :]
        for t in range(0, width, step):
            store_part(part_a, c, t, step, mm(a, w_out[:, t : t + step]))
        for u in units(c):
            line_a.rs_start(u)

    def a_reduce(c):
        for t in range(n - 1):
            for u in units(c):
                line_a.rs_step(u, t)
        for u in units(c):
            line_a.rs_own(u, own)
            start = pl.multiple_of(u * n * shard + me * shard, shard)
            hid = own[...] + tokens[pl.ds(start, shard), :].astype(F32)
            hidden_own[u] = hid
            inv = lax.rsqrt(jnp.mean(hid * hid, axis=-1, keepdims=True) + EPS)
            normed_ffn[u, me] = (hid * inv * nf[...]).astype(BF16)
            line_a.ag_start(u)

    def a_gather(c, s):
        for u in units(c):
            line_a.ag_step(u, s)

    def cot_back(c):
        k = cot[rows_of(c), :]
        for t in range(0, hidden, step):
            gact[rows_of(c), t : t + step] = mm_nt(k, w_down[t : t + step, :])

    def ffn(c):
        x = normed_ffn[pl.ds(c * HALVES, HALVES)].reshape(rows, width)
        tile = 256

        def body(i, _):
            cols = pl.ds(pl.multiple_of(i * tile, tile), tile)
            gp = mm(x, w_gate[:, cols])
            up = mm(x, w_up[:, cols])
            ga = gact[rows_of(c), cols]
            sig = jax.nn.sigmoid(gp)
            silu = gp * sig
            act[rows_of(c), cols] = (silu * up).astype(BF16)
            ggate[rows_of(c), cols] = (ga * up * sig * (1.0 + gp * (1.0 - sig))).astype(BF16)
            gup[rows_of(c), cols] = (ga * silu).astype(BF16)
            return 0

        lax.fori_loop(0, hidden // tile, body, 0)

    def ffn_back(c):
        gg, gu = ggate[rows_of(c), :], gup[rows_of(c), :]
        for t in range(0, width, step):
            store_part(
                part_c,
                c,
                t,
                step,
                mm_nt(gg, w_gate[t : t + step, :]) + mm_nt(gu, w_up[t : t + step, :]),
            )
        for u in units(c):
            line_c.rs_start(u)

    def ffn_out(c):
        a = act[rows_of(c), :]
        for t in range(0, width, step):
            store_part(ffn_part, c, t, step, mm(a, w_down[:, t : t + step]))

    def c_reduce(c):
        for t in range(n - 1):
            for u in units(c):
                line_c.rs_step(u, t)
        for u in units(c):
            line_c.rs_own(u, own)
            g = own[...]
            hid = hidden_own[u]
            start = pl.multiple_of(u * n * shard + me * shard, shard)
            inv = lax.rsqrt(jnp.mean(hid * hid, axis=-1, keepdims=True) + EPS)
            ffn_gain[...] += jnp.sum(g * hid * inv, axis=0, keepdims=True)
            scaled = g * nf[...]
            gh = (
                cot[pl.ds(start, shard), :].astype(F32)
                + inv * scaled
                - hid * (inv * inv * inv) * jnp.mean(scaled * hid, axis=-1, keepdims=True)
            )
            gh_own[u] = gh
            ghb[u, me] = gh.astype(BF16)
            line_c.ag_start(u)

    def c_gather(c, s):
        for u in units(c):
            line_c.ag_step(u, s)

    ffn_gain[...] = jnp.zeros_like(ffn_gain)
    for c in range(seqs):
        project(c)
    for c in range(seqs):
        attend(c)
        out_project(c)
        if c >= 1:
            a_reduce(c - 1)
        if c >= 2:
            for s in range(1, n):
                a_gather(c - 2, s)
    for c in range(seqs):
        cot_back(c)
        if c == 0:
            a_reduce(seqs - 1)
            if seqs >= 2:
                a_gather(seqs - 2, 1)
        elif seqs >= 2 and c + 1 < n:
            a_gather(seqs - 2, c + 1)
    if seqs >= 2:
        for s in range(seqs + 1, n):
            a_gather(seqs - 2, s)
    for c in range(seqs):
        if c == seqs - 1:
            for s in range(1, n):
                a_gather(c, s)
        ffn(c)
        ffn_back(c)
        if c >= 1:
            c_reduce(c - 1)
        if c >= 2:
            for s in range(1, n):
                c_gather(c - 2, s)
    for c in range(seqs):
        ffn_out(c)
        if c == 0:
            c_reduce(seqs - 1)
            if seqs >= 2:
                c_gather(seqs - 2, 1)
        elif seqs >= 2 and c + 1 < n:
            c_gather(seqs - 2, c + 1)
    if seqs >= 2:
        for s in range(seqs + 1, n):
            c_gather(seqs - 2, s)
    for s in range(1, n):
        c_gather(seqs - 1, s)
    for u in range(seqs * HALVES):
        line_a.rs_drain(u)
        line_a.ag_drain(u)
        line_c.rs_drain(u)
        line_c.ag_drain(u)
    for c in range(seqs):
        for d in range(1, slices):

            @pl.when(mine + d < slices)
            def _():
                kv_copy(c, d).wait_send()


def backward_kernel(
    seqs,
    tokens,
    qseg,
    kseg,
    na,
    wqkv,
    w_out,
    cos,
    sin,
    qpad,
    kv,
    lse,
    attpad,
    hidden_own,
    ffn_part,
    gh_own,
    ghb,
    block_out,
    input_grad,
    lin,
    attn_gain,
    part_b,
    rbuf_b,
    part_d,
    rbuf_d,
    own,
    dkv,
    dkv_send,
    dkv_recv,
    b_rs_s,
    b_rs_r,
    b_ag_s,
    b_ag_r,
    d_rs_s,
    d_rs_r,
    d_ag_s,
    d_ag_r,
    kv_s,
    kv_r,
):
    n = lax.axis_size("tensor")
    me = lax.axis_index("tensor")
    slices, mine = lax.axis_size("context"), lax.axis_index("context")
    rows = tokens.shape[0] // seqs
    width = tokens.shape[1]
    qw = w_out.shape[0]
    heads = qw // HEAD
    kvh = heads // 2
    pairw = wqkv.shape[1] - qw
    shard = rows // HALVES // n
    scale = 1.0 / math.sqrt(HEAD)
    line_b = Line("tensor", part_b, rbuf_b, block_out, b_rs_s, b_rs_r, b_ag_s, b_ag_r)
    line_d = Line("tensor", part_d, rbuf_d, input_grad, d_rs_s, d_rs_r, d_ag_s, d_ag_r)
    enter(True)
    step = 512

    def rows_of(c):
        return pl.ds(c * rows, rows)

    def units(c):
        return range(c * HALVES, (c + 1) * HALVES)

    def b_begin(c):
        for u in units(c):
            part_b[u] = ffn_part[u]
            line_b.rs_start(u)

    def b_reduce(c):
        for t in range(n - 1):
            for u in units(c):
                line_b.rs_step(u, t)
        for u in units(c):
            line_b.rs_own(u, own)
            block_out[u, me] = (own[...] + hidden_own[u]).astype(BF16)
            line_b.ag_start(u)

    def b_gather(c, s):
        for u in units(c):
            line_b.ag_step(u, s)

    def dkv_copy(c, d, target):
        return pltpu.make_async_remote_copy(
            src_ref=dkv_send.at[c, d - 1],
            dst_ref=dkv_recv.at[c, d - 1],
            send_sem=kv_s.at[c, d - 1],
            recv_sem=kv_r.at[c, d - 1],
            device_id={"context": target},
            device_id_type=MESH,
        )

    def attend_back(c):
        ga = mm_nt(ghb[pl.ds(c * HALVES, HALVES)].reshape(rows, width), w_out[...])
        qs = qseg[c]
        dqs = []
        bias0 = twice(mask_of(qs, kseg[c, mine], True))
        do_all = [take_head(ga, h).astype(BF16) for h in range(heads)]
        for g in range(kvh):
            do = jnp.concatenate([do_all[2 * g], do_all[2 * g + 1]], axis=0)
            att = attpad[c, 2 * g : 2 * g + 2].reshape(2 * rows, PAD)
            delta = jnp.sum(do.astype(F32) * att.astype(F32), axis=-1, keepdims=True)
            q2 = qpad[c, 2 * g : 2 * g + 2].reshape(2 * rows, PAD)
            top = lse[c, g]

            def grads(k, v, bias):
                s = mm_nt(q2, k) * scale + bias
                p = jnp.exp(s - top)
                ds = (p * (mm_nt(do, v) - delta) * scale).astype(BF16)
                return mm(ds, k), mm_tn(ds, q2), mm_tn(p.astype(BF16), do)

            dq, dk, dv = grads(kv[c, mine, g], kv[c, mine, kvh + g], bias0)
            dkv[g] = dk
            dkv[kvh + g] = dv

            def block(d, dq):
                b = mine - 1 - d
                bias = twice(mask_of(qs, kseg[c, b], False))
                more, dk, dv = grads(kv[c, b, g], kv[c, b, kvh + g], bias)
                dkv_send[c, d, g] = dk.astype(BF16)
                dkv_send[c, d, kvh + g] = dv.astype(BF16)
                return dq + more

            dq = lax.fori_loop(0, mine, block, dq)
            dqs += [dq[:rows], dq[rows:]]
        for d in range(1, slices):

            @pl.when(mine - d >= 0)
            def _():
                dkv_copy(c, d, mine - d).start()

        dq = put_heads(dqs, qw)
        ct, st = cos[rows_of(c), :], sin[rows_of(c), :]
        lin[rows_of(c), :qw] = (dq * ct - swap_halves(dq) * st).astype(BF16)
        for d in range(1, slices):

            @pl.when(mine + d < slices)
            def _():
                dkv_copy(c, d, mine + d).wait_recv()
                for h in range(2 * kvh):
                    dkv[h] = dkv[h] + dkv_recv[c, d - 1, h].astype(F32)

        p = put_heads([dkv[h] for h in range(2 * kvh)], pairw)
        back = p * ct[:, :pairw] - swap_halves(p) * st[:, :pairw]
        p = jnp.where(lane_of(p.shape) < kvh * HEAD, back, p)
        lin[rows_of(c), qw:] = p.astype(BF16)

    def d_begin(c):
        x = lin[rows_of(c), :]
        for t in range(0, width, step):
            part_d[pl.ds(c * HALVES, HALVES), :, :, t : t + step] = (
                mm_nt(x, wqkv[t : t + step, :]).astype(BF16).reshape(HALVES, n, shard, step)
            )
        for u in units(c):
            line_d.rs_start(u)

    def d_reduce(c):
        for t in range(n - 1):
            for u in units(c):
                line_d.rs_step(u, t)
        for u in units(c):
            line_d.rs_own(u, own)
            g = own[...]
            start = pl.multiple_of(u * n * shard + me * shard, shard)
            x = tokens[pl.ds(start, shard), :].astype(F32)
            inv = lax.rsqrt(jnp.mean(x * x, axis=-1, keepdims=True) + EPS)
            attn_gain[...] += jnp.sum(g * x * inv, axis=0, keepdims=True)
            scaled = g * na[...]
            input_grad[u, me] = (
                gh_own[u]
                + inv * scaled
                - x * (inv * inv * inv) * jnp.mean(scaled * x, axis=-1, keepdims=True)
            ).astype(BF16)
            line_d.ag_start(u)

    def d_gather(c, s):
        for u in units(c):
            line_d.ag_step(u, s)

    attn_gain[...] = jnp.zeros_like(attn_gain)
    for c in range(seqs):
        b_begin(c)
    for c in range(seqs):
        attend_back(c)
        d_begin(c)
        b_reduce(c)
        if c >= 1:
            d_reduce(c - 1)
            for s in range(1, n):
                b_gather(c - 1, s)
        if c >= 2:
            for s in range(1, n):
                d_gather(c - 2, s)
    d_reduce(seqs - 1)
    for s in range(1, n):
        b_gather(seqs - 1, s)
        if seqs >= 2:
            d_gather(seqs - 2, s)
    for s in range(1, n):
        d_gather(seqs - 1, s)
    for u in range(seqs * HALVES):
        line_b.rs_drain(u)
        line_b.ag_drain(u)
        line_d.rs_drain(u)
        line_d.ag_drain(u)
    for c in range(seqs):
        for d in range(1, slices):

            @pl.when(mine - d >= 0)
            def _():
                dkv_copy(c, d, mine - d).wait_send()


def rope_tables(positions, copies):
    steps = jnp.arange(HEAD // 2).astype(F32)
    inverse = THETA ** (-2.0 * steps / HEAD)
    angles = positions.astype(F32)[:, None] * inverse
    c, s = jnp.cos(angles), jnp.sin(angles)
    return (
        jnp.tile(jnp.concatenate([c, c], axis=1), (1, copies)),
        jnp.tile(jnp.concatenate([-s, s], axis=1), (1, copies)),
    )


def call(kernel, outs, scratch, ident, flops, args, out_specs=None):
    return pl.pallas_call(
        kernel,
        out_shape=outs,
        in_specs=[pl.BlockSpec(memory_space=VMEM)] * len(args),
        out_specs=[pl.BlockSpec(memory_space=VMEM)] * len(outs),
        scratch_shapes=scratch,
        compiler_params=pltpu.CompilerParams(
            collective_id=ident, has_side_effects=True, vmem_limit_bytes=67000000
        ),
        cost_estimate=pl.CostEstimate(
            flops=flops, bytes_accessed=50000000, transcendentals=0
        ),
    )(*args)


def on_device(
    tokens,
    cotangent,
    segments,
    positions,
    norm_attn,
    w_query,
    key_weight,
    value_weight,
    w_out,
    norm_ffn,
    w_gate,
    w_up,
    w_down,
):
    seqs, length, width = tokens.shape
    rows = seqs * length
    n, slices = lax.axis_size("tensor"), lax.axis_size("context")
    qw, pairw = w_query.shape[1], key_weight.shape[1] + value_weight.shape[1]
    heads, kvh = qw // HEAD, key_weight.shape[1] // HEAD
    hidden = w_gate.shape[1]
    units = seqs * HALVES
    shard = length // HALVES // n
    mine = lax.axis_index("context")

    tok = tokens.reshape(rows, width)
    cot = cotangent.reshape(rows, width)
    cos, sin = rope_tables(positions.reshape(rows), heads)
    wqkv = jnp.concatenate([w_query, key_weight, value_weight], axis=1)
    kseg = segments.reshape(seqs, slices, 1, length)
    qseg = lax.dynamic_slice_in_dim(segments, mine * length, length, 1)[..., None]
    na = norm_attn.astype(F32).reshape(1, width)
    nf = norm_ffn.astype(F32).reshape(1, width)

    def arr(shape, kind=BF16):
        return jax.ShapeDtypeStruct(shape, kind)

    line = (units, n, shard, width)
    half = (units, 2, n - 1, shard, width)
    fwd = call(
        functools.partial(forward_kernel, seqs),
        [
            arr((rows, width)),
            arr((seqs, heads, length, PAD)),
            arr((seqs, slices, 2 * kvh, length, PAD)),
            arr((seqs, kvh, 2 * length, 1), F32),
            arr((rows, qw)),
            arr((seqs, heads, length, PAD)),
            arr((units, shard, width), F32),
            arr(line),
            arr((rows, hidden)),
            arr((rows, hidden)),
            arr((rows, hidden)),
            arr(line),
            arr((units, shard, width), F32),
            arr(line),
            arr((1, width), F32),
        ],
        [
            pltpu.VMEM(line, BF16),
            pltpu.VMEM(half, BF16),
            pltpu.VMEM(line, BF16),
            pltpu.VMEM(half, BF16),
            pltpu.VMEM((rows, hidden), F32),
            pltpu.VMEM((shard, width), F32),
        ]
        + line_sems(units, n)
        + line_sems(units, n)
        + [
            pltpu.SemaphoreType.DMA((seqs, slices - 1)),
            pltpu.SemaphoreType.DMA((seqs, slices - 1)),
        ],
        0,
        2 * rows * width * (6 * hidden + 3 * qw),
        (tok, cot, qseg, kseg, na, nf, wqkv, w_out, w_gate, w_up, w_down, cos, sin),
    )
    (
        normed_attn,
        qpad,
        kv,
        lse,
        attended,
        attpad,
        hidden_own,
        normed_ffn,
        act,
        ggate,
        gup,
        ffn_part,
        gh_own,
        ghb,
        ffn_gain,
    ) = fwd
    bwd = call(
        functools.partial(backward_kernel, seqs),
        [arr(line), arr(line), arr((rows, qw + pairw)), arr((1, width), F32)],
        [
            pltpu.VMEM(line, BF16),
            pltpu.VMEM(half, BF16),
            pltpu.VMEM(line, BF16),
            pltpu.VMEM(half, BF16),
            pltpu.VMEM((shard, width), F32),
            pltpu.VMEM((2 * kvh, length, PAD), F32),
            pltpu.VMEM((seqs, slices - 1, 2 * kvh, length, PAD), BF16),
            pltpu.VMEM((seqs, slices - 1, 2 * kvh, length, PAD), BF16),
        ]
        + line_sems(units, n)
        + line_sems(units, n)
        + [
            pltpu.SemaphoreType.DMA((seqs, slices - 1)),
            pltpu.SemaphoreType.DMA((seqs, slices - 1)),
        ],
        1,
        2 * rows * width * 3 * qw,
        (
            tok,
            qseg,
            kseg,
            na,
            wqkv,
            w_out,
            cos,
            sin,
            qpad,
            kv,
            lse,
            attpad,
            hidden_own,
            ffn_part,
            gh_own,
            ghb,
        ),
    )
    block_out, input_grad, lin, attn_gain = bwd
    both = ("dp", "context")

    def summed(a, b):
        return lax.psum(mm_tn(a, b).astype(BF16), both)

    x = normed_ffn.reshape(rows, width)
    down_grad = summed(act, cot)
    gate_grad = summed(x, ggate)
    up_grad = summed(x, gup)
    out_grad = summed(attended, ghb.reshape(rows, width))
    query_grad = summed(normed_attn, lin[:, :qw])
    key_grad = summed(normed_attn, lin[:, qw : qw + pairw // 2])
    value_grad = summed(normed_attn, lin[:, qw + pairw // 2 :])
    gains = lax.psum(jnp.concatenate([attn_gain, ffn_gain]), ("dp", "context", "tensor"))
    return (
        block_out.reshape(seqs, length, width),
        input_grad.reshape(seqs, length, width),
        gains[0],
        query_grad.astype(F32),
        key_grad.astype(F32),
        value_grad.astype(F32),
        out_grad.astype(F32),
        gains[1],
        gate_grad.astype(F32),
        up_grad.astype(F32),
        down_grad.astype(F32),
    )


def solution(mesh):
    placed = (
        P("dp", "context", None),
        P("dp", "context", None),
        P("dp", None),
        P("dp", "context"),
        P(),
        P(None, "tensor"),
        P(None, "tensor"),
        P(None, "tensor"),
        P("tensor", None),
        P(),
        P(None, "tensor"),
        P(None, "tensor"),
        P("tensor", None),
    )
    return jax.shard_map(
        on_device,
        mesh=mesh,
        in_specs=placed,
        out_specs=(
            P("dp", "context", None),
            P("dp", "context", None),
            P(),
            P(None, "tensor"),
            P(None, "tensor"),
            P(None, "tensor"),
            P("tensor", None),
            P(),
            P(None, "tensor"),
            P(None, "tensor"),
            P("tensor", None),
        ),
        check_vma=False,
    )
```
